32 devices in a mesh: scene: 4 (over y, core), tile: 8 (over z, x).
Axes of the slice: x: 2, y: 2, z: 4, core: 2. Of those that a mesh axis runs over, the one named last changes fastest.
Arguments:
- node_latent: bfloat16 [131072, 128], P(('scene', 'tile')), parts along dimension 0, may hold values from -6 to 6
- cotangent: float32 [131072, 128], P(('scene', 'tile')), parts along dimension 0, may hold values from -6 to 6
- neighbours: int32 [12, 131072], P(None, ('scene', 'tile')), parts along dimension 1, may hold values from -1 to 6143, as said below
- send_rows: int32 [32, 2, 1024], P(('scene', 'tile')), parts along dimension 0, may hold values from 0 to 4095
- node_mask: int32 [131072], P(('scene', 'tile')), parts along dimension 0, may hold values 0 or 1
- w_src: bfloat16 [128, 128], replicated, may hold values from -0.5 to 0.5
- w_dst: bfloat16 [128, 128], replicated, may hold values from -0.5 to 0.5
- w_msg: bfloat16 [128, 128], replicated, may hold values from -0.5 to 0.5
- edge_gain: float32 [128], replicated, may hold values from 0.1 to 1.9
- edge_bias: float32 [128], replicated, may hold values from -3 to 3
- w_self: bfloat16 [128, 128], replicated, may hold values from -0.5 to 0.5
- w_agg: bfloat16 [128, 128], replicated, may hold values from -0.5 to 0.5
- node_bias: float32 [128], replicated, may hold values from -3 to 3
- w_out: bfloat16 [128, 128], replicated, may hold values from -0.5 to 0.5
Outputs:
- updated: bfloat16 [131072, 128], P(('scene', 'tile')), parts along dimension 0
- latent_grad: float32 [131072, 128], P(('scene', 'tile')), parts along dimension 0
- grad_src: float32 [512, 128], P('scene'), parts along dimension 0
- grad_dst: float32 [512, 128], P('scene'), parts along dimension 0
- grad_msg: float32 [512, 128], P('scene'), parts along dimension 0
- grad_edge_gain: float32 [512], P('scene'), parts along dimension 0
- grad_edge_bias: float32 [512], P('scene'), parts along dimension 0
- grad_self: float32 [512, 128], P('scene'), parts along dimension 0
- grad_agg: float32 [512, 128], P('scene'), parts along dimension 0
- grad_node_bias: float32 [512], P('scene'), parts along dimension 0
- grad_out: float32 [512, 128], P('scene'), parts along dimension 0
The draws below stay inside these ranges and needn't reach their ends.
There are 4 independent parts, one for each index of `scene`. The reference program is written for one: setup_inputs(seed, part) draws one part's arguments, and reference() takes and returns one part's arrays. A program takes and returns all parts, laid end to end along the dimension named above; an argument that names none is the same for every part. Nothing has to cross between parts.
Inputs may be any that keep to these rules, and one draw needn't show every extreme that they name: `neighbours`: each entry is -1 (empty slot) or a row of the tile's extended list: below 4096 its own nodes, then 1024 rows from the tile below, then 1024 rows from the tile above. `send_rows`: rows of the sending tile's own nodes; a row may appear more than once.
All inputs are finite; a program needn't handle non-finite values. No bound on the sum of `node_mask` on one device may be relied on, other than what follows from the above.
Results may differ from the reference program's by a relative error of at most 0.028.
Values may be sent and summed in bfloat16 or wider, within the bound.
A program may use at most 448 MiB of HBM per device.

```python
from functools import partial
import jax
import jax.numpy as jnp
from jax import lax

W = 128
DEG = 12
NDEV = 4096
HALO = 1024
TILES = 8
NODES = 32768
N_TILE = 8


def draw_neighbours(key, part):
    shape = (DEG, NODES)
    kinds = jax.random.randint(jax.random.fold_in(key, 11), shape, 0, 20)
    owned = jax.random.randint(jax.random.fold_in(key, 12), shape, 0, NDEV)
    remote = jax.random.randint(jax.random.fold_in(key, 13), shape, NDEV, NDEV + 2 * HALO)
    return jnp.where(kinds < 2, -1, jnp.where(kinds < 5, remote, owned)).astype(jnp.int32)


def set_ends(array, key, low, high):
    index_at = [jax.random.randint(jax.random.fold_in(key, axis), (), 0, length) for axis, length in enumerate(array.shape)]
    longest = array.shape.index(max(array.shape))
    beside = index_at[:longest] + [(index_at[longest] + 1) % array.shape[longest]] + index_at[longest + 1:]
    return array.at[tuple(index_at)].set(low).at[tuple(beside)].set(high)


def level_of(key, extent, cuts, smallest, top_value):
    def one(dim, parts):
        steps = jax.random.uniform(jax.random.fold_in(jax.random.fold_in(key, 6), dim), (parts,), jnp.float32, smallest / len(cuts), top_value / len(cuts))
        return jnp.repeat(jnp.exp(steps), extent[dim] // parts).reshape((-1,) + (1,) * (len(extent) - dim - 1))

    level = one(*cuts[0])
    for cut in cuts[1:]:
        level = level * one(*cut)
    return level


def gaussian(own_key, shape, deviation, bound, split=(), dtype=jnp.bfloat16):
    entries = jax.random.normal(own_key, shape, jnp.float32) * deviation
    if len(split) > 0:
        entries = level_of(own_key, shape, split, -0.22, 0.18) * entries
    return jnp.clip(entries, min=-bound, max=bound).astype(dtype)


def setup_inputs(seed: int = 0, part: int = 0) -> dict:
    streams_of = jax.random.split(jax.random.key(seed), 15)
    part_keys = jax.random.split(jax.random.fold_in(streams_of[14], part), 15)
    node_latent = gaussian(part_keys[0], (NODES, W), 1.0, 6.0, ((0, 8),))
    cotangent = gaussian(part_keys[1], (NODES, W), 1.0, 6.0, ((0, 8),), jnp.float32)
    neighbours = draw_neighbours(jax.random.fold_in(jax.random.fold_in(streams_of[14], part), 71), part)
    send_rows = set_ends(jax.random.randint(part_keys[3], (TILES, 2, HALO), 0, NDEV), jax.random.fold_in(part_keys[3], 1), 0, NDEV - 1).astype(jnp.int32)
    node_mask = set_ends((jax.random.randint(part_keys[4], (NODES,), 0, 4) < 3).astype(jnp.int32), jax.random.fold_in(part_keys[4], 1), 0, 1)
    w_src = gaussian(streams_of[5], (W, W), W ** -0.5, 0.5)
    w_dst = gaussian(streams_of[6], (W, W), W ** -0.5, 0.5)
    w_msg = gaussian(streams_of[7], (W, W), W ** -0.5, 0.5)
    edge_gain = jnp.clip(1.0 + 0.18 * jax.random.normal(streams_of[8], (W,), jnp.float32), 0.1, 1.9)
    edge_bias = gaussian(streams_of[9], (W,), 0.5, 3.0, (), jnp.float32)
    w_self = gaussian(streams_of[10], (W, W), W ** -0.5, 0.5)
    w_agg = gaussian(streams_of[11], (W, W), W ** -0.5, 0.5)
    node_bias = gaussian(streams_of[12], (W,), 0.5, 3.0, (), jnp.float32)
    w_out = gaussian(streams_of[13], (W, W), W ** -0.5, 0.5)
    return dict(node_latent=node_latent, cotangent=cotangent, neighbours=neighbours, send_rows=send_rows, node_mask=node_mask, w_src=w_src, w_dst=w_dst, w_msg=w_msg, edge_gain=edge_gain, edge_bias=edge_bias, w_self=w_self, w_agg=w_agg, node_bias=node_bias, w_out=w_out)


def edge_block(w_msg, edge_gain, proj_src, pieces):
    source, proj_part = pieces
    present = (source >= 0)[:, :, None]
    gathered = proj_src[jnp.maximum(source, 0)] + proj_part[None]
    hidden = jax.nn.silu(gathered).astype(jnp.bfloat16)
    degree, block_rows, feature = hidden.shape
    message = jnp.dot(hidden.reshape(degree * block_rows, feature), w_msg.astype(jnp.bfloat16), preferred_element_type=jnp.float32)
    message = message.reshape(degree, block_rows, feature)
    centre = lax.optimization_barrier(jnp.mean(message, axis=2, keepdims=True))
    spread = lax.optimization_barrier(jnp.mean(jnp.square(message - centre), axis=2, keepdims=True))
    normed = (message - centre) * lax.rsqrt(spread + 1e-05) * edge_gain
    return lax.optimization_barrier(jnp.sum(jnp.where(present, normed, 0.0), axis=0))

def edge_section(eparams, extended32, neighbours, again):
    w_src, w_dst, w_msg, edge_gain, edge_bias = eparams
    degree, node_count = neighbours.shape
    extended = extended32.astype(jnp.bfloat16)
    proj_src = jnp.dot(extended, w_src.astype(jnp.bfloat16), preferred_element_type=jnp.float32)
    proj_dst = jnp.dot(extended[:node_count], w_dst.astype(jnp.bfloat16), preferred_element_type=jnp.float32) + edge_bias
    block_rows = min(node_count, 1024)
    nblocks = node_count // block_rows
    groups = neighbours.reshape(degree, nblocks, block_rows).transpose(1, 0, 2)
    worker = partial(edge_block, w_msg, edge_gain, proj_src)
    if again:
        worker = jax.checkpoint(worker)
    summed = lax.map(worker, (groups, proj_dst.reshape(nblocks, block_rows, -1)))
    return summed.reshape(node_count, -1)

def node_section(nparams, own32, summed_bf, node_mask):
    w_self, w_agg, node_bias, w_out = nparams
    own = own32.astype(jnp.bfloat16)
    inner = jnp.dot(own, w_self.astype(jnp.bfloat16), preferred_element_type=jnp.float32)
    inner = inner + jnp.dot(summed_bf, w_agg.astype(jnp.bfloat16), preferred_element_type=jnp.float32) + node_bias
    update = jax.nn.silu(inner).astype(jnp.bfloat16)
    return own32 + node_mask.astype(jnp.float32)[:, None] * jnp.dot(update, w_out.astype(jnp.bfloat16), preferred_element_type=jnp.float32)

def tile_forward(params, extended32, neighbours, node_mask):
    node_count = neighbours.shape[1]
    summed = edge_section(params[:5], extended32, neighbours, False)
    return node_section(params[5:], extended32[:node_count], summed.astype(jnp.bfloat16), node_mask)

def reference(node_latent, cotangent, neighbours, send_rows, node_mask, w_src, w_dst, w_msg, edge_gain, edge_bias, w_self, w_agg, node_bias, w_out):
    params = tuple((p.astype(jnp.float32) for p in (w_src, w_dst, w_msg, edge_gain, edge_bias, w_self, w_agg, node_bias, w_out)))
    latent32 = node_latent.astype(jnp.float32)
    tiled_nbr = neighbours.reshape(DEG, N_TILE, NDEV).transpose(1, 0, 2)
    tiled_mask = node_mask.reshape(N_TILE, NDEV)

    def scene(params, latent32):
        tiled = latent32.reshape(N_TILE, NDEV, W)
        down_send = jax.vmap(lambda block, listing: block[listing])(tiled, send_rows[:, 0])
        up_send = jax.vmap(lambda block, listing: block[listing])(tiled, send_rows[:, 1])
        extended = jnp.concatenate([tiled, jnp.roll(up_send, 1, axis=0), jnp.roll(down_send, -1, axis=0)], axis=1)

        def one_tile(pieces):
            return tile_forward(params, pieces[0], pieces[1], pieces[2])
        result = lax.map(jax.checkpoint(one_tile), (extended, tiled_nbr, tiled_mask))
        return result.reshape(NODES, W)
    result, backward = jax.vjp(scene, params, latent32)
    grads, latent_grad = backward(cotangent)
    factor = NODES ** (-0.5)
    grads = tuple((g * factor for g in grads))
    return (result.astype(jnp.bfloat16), latent_grad, grads[0], grads[1], grads[2], grads[3], grads[4], grads[5], grads[6], grads[7], grads[8])
```

```python
import functools

import jax
import jax.numpy as jnp
from jax import lax
from jax.experimental import pallas as pl
from jax.experimental.pallas import tpu as pltpu
from jax.sharding import PartitionSpec as P

BLOCK = 128
COPIES = 8
BF = jnp.bfloat16
F32 = jnp.float32


def mm(a, b):
    return jnp.dot(a, b, preferred_element_type=F32)


def mm_nt(a, b):
    return lax.dot_general(a, b, (((1,), (1,)), ((), ())), preferred_element_type=F32)


def mm_tn(a, b):
    return lax.dot_general(a, b, (((0,), (0,)), ((), ())), preferred_element_type=F32)


def sigmoid(x):
    return 0.5 * jnp.tanh(0.5 * x) + 0.5


def layer_kernel(
    degree,
    idx_ref,
    own_ref,
    ct_ref,
    cols_ref,
    ext_ref,
    w_src_ref,
    w_dst_ref,
    w_msg_ref,
    w_cent_ref,
    gain_ref,
    ebias_ref,
    w_self_ref,
    w_agg_ref,
    nbias_ref,
    w_out_ref,
    updated_ref,
    down_ref,
    dext_ref,
    gw_ref,
    gv_ref,
    table,
    rows,
    hid,
    slope,
    yhat,
    rstd,
    dmsg,
    *accs,
):
    step = pl.program_id(0)
    count = own_ref.shape[0]
    width = own_ref.shape[1]
    copies = len(accs)
    edges = degree * count
    unroll = 2 * copies

    @pl.when(step == 0)
    def _():
        table[...] = mm(ext_ref[...], w_src_ref[...])
        for acc in accs:
            acc[...] = jnp.zeros_like(acc)
        gw_ref[...] = jnp.zeros_like(gw_ref)
        gv_ref[...] = jnp.zeros_like(gv_ref)

    def gather(t, carry):
        base = pl.multiple_of(t * unroll, unroll)
        for j in range(unroll):
            i = idx_ref[0, 0, base + j]
            rows[pl.ds(base + j, 1), :] = table[pl.ds(i, 1), :]
        return carry

    lax.fori_loop(0, edges // unroll, gather, 0)

    own = own_ref[...]
    ones = jnp.full((width, width), 1.0 / width, BF)
    gain = gain_ref[...]
    pd = mm(own, w_dst_ref[...]) + ebias_ref[...]
    cols = cols_ref[...]

    def present(k):
        return jnp.broadcast_to((cols[:, k : k + 1] >= 0).astype(F32), (count, width))

    ysum = jnp.zeros((count, width), F32)
    for k in range(degree):
        at = pl.ds(k * count, count)
        x = rows[at, :] + pd
        s = sigmoid(x)
        h = x * s
        hb = h.astype(BF)
        hid[at, :] = hb
        slope[at, :] = s + h - h * s
        c = mm(hb, w_cent_ref[...])
        var = mm((c * c).astype(BF), ones)
        r = lax.rsqrt(var + 1e-5)
        y = c * r
        m = present(k)
        yhat[at, :] = y
        rstd[at, :] = r * m
        ysum = ysum + y * m

    sb = (ysum * gain).astype(BF)
    pre = mm(own, w_self_ref[...]) + mm(sb, w_agg_ref[...]) + nbias_ref[...]
    s = sigmoid(pre)
    u = pre * s
    ub = u.astype(BF)
    live = jnp.broadcast_to(cols[:, degree : degree + 1], (count, width)).astype(F32)
    ct = ct_ref[...]
    updated_ref[...] = (own.astype(F32) + live * mm(ub, w_out_ref[...])).astype(BF)
    dob = (live * ct).astype(BF)
    dpre = mm_nt(dob, w_out_ref[...]) * (s + u - u * s)
    dpb = dpre.astype(BF)
    dsum = mm_nt(dpb, w_agg_ref[...])
    dy = dsum * gain
    dyc = dy - jnp.mean(dy, axis=1, keepdims=True)

    dpd = jnp.zeros((count, width), F32)
    for k in range(degree):
        at = pl.ds(k * count, count)
        y = yhat[at, :]
        t = mm((dyc * y).astype(BF), ones)
        dm = (rstd[at, :] * (dyc - y * t)).astype(BF)
        dmsg[at, :] = dm
        dx = mm_nt(dm, w_msg_ref[...]) * slope[at, :]
        rows[at, :] = dx
        dpd = dpd + dx

    dpdb = dpd.astype(BF)
    down_ref[...] = ct + mm_nt(dpb, w_self_ref[...]) + mm_nt(dpdb, w_dst_ref[...])
    gw_ref[1] += mm_tn(own, dpdb)
    gw_ref[2] += mm_tn(hid[...], dmsg[...])
    gw_ref[3] += mm_tn(own, dpb)
    gw_ref[4] += mm_tn(sb, dpb)
    gw_ref[5] += mm_tn(ub, dob)
    gv_ref[0:1] += jnp.sum(dsum * ysum, axis=0, keepdims=True)
    gv_ref[1:2] += jnp.sum(dpd, axis=0, keepdims=True)
    gv_ref[2:3] += jnp.sum(dpre, axis=0, keepdims=True)

    def scatter(t, carry):
        base = pl.multiple_of(t * unroll, unroll)
        for first in range(0, unroll, copies):
            where = [idx_ref[0, 0, base + first + j] for j in range(copies)]
            total = [
                accs[j][pl.ds(where[j], 1), :] + rows[pl.ds(base + first + j, 1), :]
                for j in range(copies)
            ]
            for j in range(copies):
                accs[j][pl.ds(where[j], 1), :] = total[j]
        return carry

    lax.fori_loop(0, edges // unroll, scatter, 0)

    @pl.when(step == pl.num_programs(0) - 1)
    def _():
        dproj = accs[0][...]
        for acc in accs[1:]:
            dproj = dproj + acc[...]
        dpb = dproj.astype(BF)
        dext_ref[...] = mm_nt(dpb, w_src_ref[...])
        gw_ref[0] = mm_tn(ext_ref[...], dpb)


def layer(extended, node_latent, cotangent, neighbours, node_mask, weights):
    w_src, w_dst, w_msg, edge_gain, edge_bias, w_self, w_agg, node_bias, w_out = weights
    degree, nodes = neighbours.shape
    width = node_latent.shape[1]
    listed = extended.shape[0]
    count = min(BLOCK, nodes)
    blocks = nodes // count
    idx = jnp.maximum(neighbours, 0).reshape(degree, blocks, count)
    idx = idx.transpose(1, 0, 2).reshape(blocks, 1, degree * count)
    cols = jnp.concatenate([neighbours, node_mask[None]], axis=0).T
    w32 = w_msg.astype(F32)
    w_cent = (w32 - jnp.mean(w32, axis=1, keepdims=True)).astype(BF)
    whole = lambda shape: pl.BlockSpec(shape, lambda i: (0,) * len(shape))
    mat = whole((width, width))
    vec = whole((1, width))
    rowed = pl.BlockSpec((count, width), lambda i: (i, 0))
    edges = degree * count
    return pl.pallas_call(
        functools.partial(layer_kernel, degree),
        grid=(blocks,),
        in_specs=[
            pl.BlockSpec((1, 1, edges), lambda i: (i, 0, 0), memory_space=pltpu.SMEM),
            rowed,
            rowed,
            pl.BlockSpec((count, degree + 1), lambda i: (i, 0)),
            whole((listed, width)),
            mat,
            mat,
            mat,
            mat,
            vec,
            vec,
            mat,
            mat,
            vec,
            mat,
        ],
        out_specs=[
            rowed,
            rowed,
            whole((listed, width)),
            whole((6, width, width)),
            whole((8, width)),
        ],
        out_shape=[
            jax.ShapeDtypeStruct((nodes, width), BF),
            jax.ShapeDtypeStruct((nodes, width), F32),
            jax.ShapeDtypeStruct((listed, width), F32),
            jax.ShapeDtypeStruct((6, width, width), F32),
            jax.ShapeDtypeStruct((8, width), F32),
        ],
        scratch_shapes=[
            pltpu.VMEM((listed, width), F32),
            pltpu.VMEM((edges, width), F32),
            pltpu.VMEM((edges, width), BF),
            pltpu.VMEM((edges, width), F32),
            pltpu.VMEM((edges, width), F32),
            pltpu.VMEM((edges, width), F32),
            pltpu.VMEM((edges, width), BF),
        ]
        + [pltpu.VMEM((listed, width), F32)] * COPIES,
        compiler_params=pltpu.CompilerParams(
            dimension_semantics=("arbitrary",), vmem_limit_bytes=60 * 2**20
        ),
        name="layer",
    )(
        idx,
        node_latent,
        cotangent,
        cols,
        extended,
        w_src,
        w_dst,
        w_msg,
        w_cent,
        edge_gain[None],
        edge_bias[None],
        w_self,
        w_agg,
        node_bias[None],
        w_out,
    )


def finish_kernel(list_ref, back_ref, dext_ref, down_ref, out_ref):
    count = out_ref.shape[0]
    first = pl.program_id(0) * count
    total = dext_ref[...] + down_ref[...]
    span = list_ref.shape[1]
    here = lax.broadcasted_iota(jnp.int32, (count, span), 0) + first
    hit = jnp.where(here == list_ref[...], 1.0, 0.0).astype(BF)
    out_ref[...] = total + mm(hit, back_ref[...])


def finish(listing, back, dext, down):
    nodes, width = down.shape
    count = min(512, nodes)
    rowed = pl.BlockSpec((count, width), lambda i: (i, 0))
    return pl.pallas_call(
        finish_kernel,
        grid=(nodes // count,),
        in_specs=[
            pl.BlockSpec((1, listing.shape[1]), lambda i: (0, 0)),
            pl.BlockSpec(back.shape, lambda i: (0, 0)),
            rowed,
            rowed,
        ],
        out_specs=rowed,
        out_shape=jax.ShapeDtypeStruct((nodes, width), F32),
        compiler_params=pltpu.CompilerParams(
            dimension_semantics=("arbitrary",), vmem_limit_bytes=60 * 2**20
        ),
        name="finish",
    )(listing, back, dext, down)


def on_device(node_latent, cotangent, neighbours, send_rows, node_mask, *weights):
    nodes = node_latent.shape[0]
    rim = send_rows.shape[2]
    size = lax.axis_size("tile")
    up = [(i, (i + 1) % size) for i in range(size)]
    down = [(j, i) for i, j in up]
    listing = send_rows.reshape(1, 2 * rim)
    outbound = node_latent[listing[0]]
    before = lax.ppermute(outbound[rim:], "tile", up)
    after = lax.ppermute(outbound[:rim], "tile", down)
    extended = jnp.concatenate([node_latent, before, after], axis=0)
    updated, down_grad, dext, gw, gv = layer(
        extended, node_latent, cotangent, neighbours, node_mask, weights
    )
    halo = dext[nodes:].astype(BF)
    to_below = lax.ppermute(halo[:rim], "tile", down)
    to_above = lax.ppermute(halo[rim:], "tile", up)
    back = jnp.concatenate([to_above, to_below], axis=0)
    packed = jnp.concatenate([gw.reshape(-1, gw.shape[2]), gv], axis=0).astype(BF)
    packed = lax.psum(packed, "tile").astype(F32)
    latent_grad = finish(listing, back, dext, down_grad)
    packed = packed * (nodes * size) ** (-0.5)
    width = gw.shape[2]
    mats = [packed[i * width : (i + 1) * width] for i in range(6)]
    vecs = [packed[6 * width + i] for i in range(3)]
    return (
        updated,
        latent_grad,
        mats[0],
        mats[1],
        mats[2],
        vecs[0],
        vecs[1],
        mats[3],
        mats[4],
        vecs[2],
        mats[5],
    )


def solution(mesh):
    rowed, shared = P(("scene", "tile"), None), P()
    in_specs = (
        rowed,
        rowed,
        P(None, ("scene", "tile")),
        P(("scene", "tile"), None, None),
        P(("scene", "tile")),
    ) + (shared,) * 9
    mat, vec = P("scene", None), P("scene")
    out_specs = (rowed, rowed, mat, mat, mat, vec, vec, mat, mat, vec, mat)
    return jax.shard_map(
        on_device, mesh=mesh, in_specs=in_specs, out_specs=out_specs, check_vma=False
    )
```

```python
import functools

import jax
import jax.numpy as jnp
from jax import lax
from jax.experimental import pallas as pl
from jax.experimental.pallas import tpu as pltpu
from jax.sharding import PartitionSpec as P

BLOCK = 128
COPIES = 12
BF = jnp.bfloat16
F32 = jnp.float32


def mm(a, b):
    return jnp.dot(a, b, preferred_element_type=F32)


def mm_nt(a, b):
    return lax.dot_general(a, b, (((1,), (1,)), ((), ())), preferred_element_type=F32)


def mm_tn(a, b):
    return lax.dot_general(a, b, (((0,), (0,)), ((), ())), preferred_element_type=F32)


def sigmoid(x):
    return 0.5 * jnp.tanh(0.5 * x) + 0.5


def layer_kernel(
    degree,
    idx_ref,
    own_ref,
    ct_ref,
    cols_ref,
    ext_ref,
    w_src_ref,
    w_dst_ref,
    w_msg_ref,
    w_cent_ref,
    gain_ref,
    ebias_ref,
    w_self_ref,
    w_agg_ref,
    nbias_ref,
    w_out_ref,
    updated_ref,
    down_ref,
    dext_ref,
    gw_ref,
    gv_ref,
    table,
    rows,
    hid,
    slope,
    yhat,
    rstd,
    dmsg,
    *accs,
):
    step = pl.program_id(0)
    count = own_ref.shape[0]
    width = own_ref.shape[1]
    copies = len(accs)
    edges = degree * count
    unroll = 4 * copies

    @pl.when(step == 0)
    def _():
        table[...] = mm(ext_ref[...], w_src_ref[...])
        for acc in accs:
            acc[...] = jnp.zeros_like(acc)
        gw_ref[...] = jnp.zeros_like(gw_ref)
        gv_ref[...] = jnp.zeros_like(gv_ref)

    def gather(t, carry):
        base = pl.multiple_of(t * unroll, unroll)
        for j in range(unroll):
            i = idx_ref[0, 0, base + j]
            rows[pl.ds(base + j, 1), :] = table[pl.ds(i, 1), :]
        return carry

    lax.fori_loop(0, edges // unroll, gather, 0)

    own = own_ref[...]
    ones = jnp.full((width, width), 1.0 / width, BF)
    gain = gain_ref[...]
    pd = mm(own, w_dst_ref[...]) + ebias_ref[...]
    cols = cols_ref[...]

    def present(k):
        return jnp.broadcast_to((cols[:, k : k + 1] >= 0).astype(F32), (count, width))

    ysum = jnp.zeros((count, width), F32)
    for k in range(degree):
        at = pl.ds(k * count, count)
        x = rows[at, :] + pd
        s = sigmoid(x)
        h = x * s
        hb = h.astype(BF)
        hid[at, :] = hb
        slope[at, :] = s + h - h * s
        c = mm(hb, w_cent_ref[...])
        var = mm((c * c).astype(BF), ones)
        r = lax.rsqrt(var + 1e-5)
        y = c * r
        m = present(k)
        yhat[at, :] = y
        rstd[at, :] = r * m
        ysum = ysum + y * m

    sb = (ysum * gain).astype(BF)
    pre = mm(own, w_self_ref[...]) + mm(sb, w_agg_ref[...]) + nbias_ref[...]
    s = sigmoid(pre)
    u = pre * s
    ub = u.astype(BF)
    live = jnp.broadcast_to(cols[:, degree : degree + 1], (count, width)).astype(F32)
    ct = ct_ref[...]
    updated_ref[...] = (own.astype(F32) + live * mm(ub, w_out_ref[...])).astype(BF)
    dob = (live * ct).astype(BF)
    dpre = mm_nt(dob, w_out_ref[...]) * (s + u - u * s)
    dpb = dpre.astype(BF)
    dsum = mm_nt(dpb, w_agg_ref[...])
    dy = dsum * gain
    dyc = dy - jnp.mean(dy, axis=1, keepdims=True)

    dpd = jnp.zeros((count, width), F32)
    for k in range(degree):
        at = pl.ds(k * count, count)
        y = yhat[at, :]
        t = mm((dyc * y).astype(BF), ones)
        dm = (rstd[at, :] * (dyc - y * t)).astype(BF)
        dmsg[at, :] = dm
        dx = mm_nt(dm, w_msg_ref[...]) * slope[at, :]
        rows[at, :] = dx
        dpd = dpd + dx

    dpdb = dpd.astype(BF)
    down_ref[...] = ct + mm_nt(dpb, w_self_ref[...]) + mm_nt(dpdb, w_dst_ref[...])
    gw_ref[1] += mm_tn(own, dpdb)
    gw_ref[2] += mm_tn(hid[...], dmsg[...])
    gw_ref[3] += mm_tn(own, dpb)
    gw_ref[4] += mm_tn(sb, dpb)
    gw_ref[5] += mm_tn(ub, dob)
    gv_ref[0:1] += jnp.sum(dsum * ysum, axis=0, keepdims=True)
    gv_ref[1:2] += jnp.sum(dpd, axis=0, keepdims=True)
    gv_ref[2:3] += jnp.sum(dpre, axis=0, keepdims=True)

    def scatter(t, carry):
        base = pl.multiple_of(t * unroll, unroll)
        for first in range(0, unroll, copies):
            where = [idx_ref[0, 0, base + first + j] for j in range(copies)]
            total = [
                accs[j][pl.ds(where[j], 1), :] + rows[pl.ds(base + first + j, 1), :]
                for j in range(copies)
            ]
            for j in range(copies):
                accs[j][pl.ds(where[j], 1), :] = total[j]
        return carry

    lax.fori_loop(0, edges // unroll, scatter, 0)

    @pl.when(step == pl.num_programs(0) - 1)
    def _():
        dproj = accs[0][...]
        for acc in accs[1:]:
            dproj = dproj + acc[...]
        dpb = dproj.astype(BF)
        dext_ref[...] = mm_nt(dpb, w_src_ref[...])
        gw_ref[0] = mm_tn(ext_ref[...], dpb)


def layer(extended, node_latent, cotangent, neighbours, node_mask, weights):
    w_src, w_dst, w_msg, edge_gain, edge_bias, w_self, w_agg, node_bias, w_out = weights
    degree, nodes = neighbours.shape
    width = node_latent.shape[1]
    listed = extended.shape[0]
    count = min(BLOCK, nodes)
    blocks = nodes // count
    idx = jnp.maximum(neighbours, 0).reshape(degree, blocks, count)
    idx = idx.transpose(1, 0, 2).reshape(blocks, 1, degree * count)
    cols = jnp.concatenate([neighbours, node_mask[None]], axis=0).T
    w32 = w_msg.astype(F32)
    w_cent = (w32 - jnp.mean(w32, axis=1, keepdims=True)).astype(BF)
    whole = lambda shape: pl.BlockSpec(shape, lambda i: (0,) * len(shape))
    mat = whole((width, width))
    vec = whole((1, width))
    rowed = pl.BlockSpec((count, width), lambda i: (i, 0))
    edges = degree * count
    return pl.pallas_call(
        functools.partial(layer_kernel, degree),
        grid=(blocks,),
        in_specs=[
            pl.BlockSpec((1, 1, edges), lambda i: (i, 0, 0), memory_space=pltpu.SMEM),
            rowed,
            rowed,
            pl.BlockSpec((count, degree + 1), lambda i: (i, 0)),
            whole((listed, width)),
            mat,
            mat,
            mat,
            mat,
            vec,
            vec,
            mat,
            mat,
            vec,
            mat,
        ],
        out_specs=[
            rowed,
            rowed,
            whole((listed, width)),
            whole((6, width, width)),
            whole((8, width)),
        ],
        out_shape=[
            jax.ShapeDtypeStruct((nodes, width), BF),
            jax.ShapeDtypeStruct((nodes, width), F32),
            jax.ShapeDtypeStruct((listed, width), F32),
            jax.ShapeDtypeStruct((6, width, width), F32),
            jax.ShapeDtypeStruct((8, width), F32),
        ],
        scratch_shapes=[
            pltpu.VMEM((listed, width), F32),
            pltpu.VMEM((edges, width), F32),
            pltpu.VMEM((edges, width), BF),
            pltpu.VMEM((edges, width), F32),
            pltpu.VMEM((edges, width), F32),
            pltpu.VMEM((edges, width), F32),
            pltpu.VMEM((edges, width), BF),
        ]
        + [pltpu.VMEM((listed, width), F32)] * COPIES,
        compiler_params=pltpu.CompilerParams(
            dimension_semantics=("arbitrary",), vmem_limit_bytes=60 * 2**20
        ),
        name="layer",
    )(
        idx,
        node_latent,
        cotangent,
        cols,
        extended,
        w_src,
        w_dst,
        w_msg,
        w_cent,
        edge_gain[None],
        edge_bias[None],
        w_self,
        w_agg,
        node_bias[None],
        w_out,
    )


def finish_kernel(list_ref, back_ref, dext_ref, down_ref, out_ref):
    count = out_ref.shape[0]
    first = pl.program_id(0) * count
    total = dext_ref[...] + down_ref[...]
    span = list_ref.shape[1]
    here = lax.broadcasted_iota(jnp.int32, (count, span), 0) + first
    hit = jnp.where(here == list_ref[...], 1.0, 0.0).astype(BF)
    out_ref[...] = total + mm(hit, back_ref[...])


def finish(listing, back, dext, down):
    nodes, width = down.shape
    count = min(512, nodes)
    rowed = pl.BlockSpec((count, width), lambda i: (i, 0))
    return pl.pallas_call(
        finish_kernel,
        grid=(nodes // count,),
        in_specs=[
            pl.BlockSpec((1, listing.shape[1]), lambda i: (0, 0)),
            pl.BlockSpec(back.shape, lambda i: (0, 0)),
            rowed,
            rowed,
        ],
        out_specs=rowed,
        out_shape=jax.ShapeDtypeStruct((nodes, width), F32),
        compiler_params=pltpu.CompilerParams(
            dimension_semantics=("arbitrary",), vmem_limit_bytes=60 * 2**20
        ),
        name="finish",
    )(listing, back, dext, down)


def total_over(value, axis):
    size = lax.axis_size(axis)
    if size & (size - 1):
        return lax.psum(value, axis)
    bit = 1
    while bit < size:
        other = lax.ppermute(value, axis, [(i, i ^ bit) for i in range(size)])
        value = (value.astype(F32) + other.astype(F32)).astype(BF)
        bit *= 2
    return value


def on_device(node_latent, cotangent, neighbours, send_rows, node_mask, *weights):
    nodes = node_latent.shape[0]
    rim = send_rows.shape[2]
    size = lax.axis_size("tile")
    up = [(i, (i + 1) % size) for i in range(size)]
    down = [(j, i) for i, j in up]
    listing = send_rows.reshape(1, 2 * rim)
    outbound = node_latent[listing[0]]
    before = lax.ppermute(outbound[rim:], "tile", up)
    after = lax.ppermute(outbound[:rim], "tile", down)
    extended = jnp.concatenate([node_latent, before, after], axis=0)
    updated, down_grad, dext, gw, gv = layer(
        extended, node_latent, cotangent, neighbours, node_mask, weights
    )
    halo = dext[nodes:].astype(BF)
    to_below = lax.ppermute(halo[:rim], "tile", down)
    to_above = lax.ppermute(halo[rim:], "tile", up)
    back = jnp.concatenate([to_above, to_below], axis=0)
    packed = jnp.concatenate([gw.reshape(-1, gw.shape[2]), gv], axis=0).astype(BF)
    packed = total_over(packed, "tile").astype(F32)
    latent_grad = finish(listing, back, dext, down_grad)
    packed = packed * (nodes * size) ** (-0.5)
    width = gw.shape[2]
    mats = [packed[i * width : (i + 1) * width] for i in range(6)]
    vecs = [packed[6 * width + i] for i in range(3)]
    return (
        updated,
        latent_grad,
        mats[0],
        mats[1],
        mats[2],
        vecs[0],
        vecs[1],
        mats[3],
        mats[4],
        vecs[2],
        mats[5],
    )


def solution(mesh):
    rowed, shared = P(("scene", "tile"), None), P()
    in_specs = (
        rowed,
        rowed,
        P(None, ("scene", "tile")),
        P(("scene", "tile"), None, None),
        P(("scene", "tile")),
    ) + (shared,) * 9
    mat, vec = P("scene", None), P("scene")
    out_specs = (rowed, rowed, mat, mat, mat, vec, vec, mat, mat, vec, mat)
    return jax.shard_map(
        on_device, mesh=mesh, in_specs=in_specs, out_specs=out_specs, check_vma=False
    )
```
